256 devices in a mesh: row: 16 (over z, y_hi), col: 16 (over y_lo, x, core).
Axes of the slice: x: 4, y: 4 (y_hi: 2, y_lo: 2; y = y_hi * 2 + y_lo), z: 8, core: 2. Of those that a mesh axis runs over, the one named last changes fastest.
Arguments:
- inputs: bfloat16 [512, 8192], P('col', 'row'), may hold values from -6 to 6
- cotangent: bfloat16 [512, 8192], P('col', 'row'), may hold values from -1.59375 to 1.59375
- weight_in: bfloat16 [8192, 32768], P('row', 'col'), may hold values from -0.125 to 0.125
- weight_out: bfloat16 [32768, 8192], P('col', 'row'), may hold values from -0.0625 to 0.0625
- mask_in: int32 [64, 256], P('row', 'col'), may hold values 0 or 1
- mask_out: int32 [256, 64], P('col', 'row'), may hold values 0 or 1
Outputs:
- grad_inputs: float32 [512, 8192], P('col', 'row')
- grad_weight_in: float32 [8192, 32768], P('row', 'col')
- grad_weight_out: float32 [32768, 8192], P('col', 'row')
The draws below stay inside these ranges and needn't reach their ends.
All inputs are finite; a program needn't handle non-finite values. No bound on the sum of `mask_in` or of `mask_out` on one device may be relied on, other than what follows from the above.
Results may differ from the reference program's by a relative error of at most 0.0029.
Values may be sent and summed in bfloat16 or wider, within the bound.
No kernel may reach another device: no remote copies, remote signals or barrier semaphores. Data moves between devices by JAX's collectives and lax.ppermute only.
A program may use at most 128 MiB of HBM per device.

```python
import jax
import jax.numpy as jnp
from jax import lax

D = 8192
H = 32768
BLOCK = 128
TOKENS = 512


def place_ends(entries, stream_key, least, largest):
    place = [jax.random.randint(jax.random.fold_in(stream_key, axis), (), 0, length) for axis, length in enumerate(entries.shape)]
    longest = entries.shape.index(max(entries.shape))
    neighbour = place[:longest] + [(place[longest] + 1) % entries.shape[longest]] + place[longest + 1:]
    return entries.at[tuple(place)].set(least).at[tuple(neighbour)].set(largest)


def steps_of(stream_key, dims, pieces, smallest, top_value):
    level, own = 1.0, jax.random.fold_in(stream_key, 6)
    for dim, shards_of in pieces:
        heights = jnp.exp(jax.random.uniform(jax.random.fold_in(own, dim), (shards_of,), jnp.float32, smallest / len(pieces), top_value / len(pieces)))
        level = level * jnp.repeat(heights, dims[dim] // shards_of).reshape([-1 if axis == dim else 1 for axis in range(len(dims))])
    return level


def centred(rng, dims, scale, reach, pieces=(), held_as=jnp.bfloat16):
    level = steps_of(rng, dims, pieces, -0.22, 0.18) if pieces else 1.0
    values = jax.random.normal(rng, dims, jnp.float32) * scale * level
    return jnp.minimum(jnp.maximum(values, -reach), reach).astype(held_as)


def setup_inputs(seed: int = 0) -> dict:
    arg_keys = jax.random.split(jax.random.key(seed), 7)
    inputs = centred(arg_keys[0], (TOKENS, D), 1.0, 6.0, ((0, 16), (1, 16)))
    cotangent = centred(arg_keys[1], (TOKENS, D), 0.2, 1.59375, ((0, 16), (1, 16)))
    weight_in = centred(arg_keys[2], (D, H), (D // 4) ** -0.5, 0.125, ((0, 16), (1, 16)))
    weight_out = centred(arg_keys[3], (H, D), (H // 4) ** -0.5, 0.0625, ((0, 16), (1, 16)))
    mask_in = place_ends((jax.random.randint(arg_keys[4], (D // BLOCK, H // BLOCK), 0, 4) < 1).astype(jnp.int32), jax.random.fold_in(arg_keys[4], 1), 0, 1)
    mask_out = place_ends((jax.random.randint(arg_keys[5], (H // BLOCK, D // BLOCK), 0, 4) < 1).astype(jnp.int32), jax.random.fold_in(arg_keys[5], 1), 0, 1)
    return dict(inputs=inputs, cotangent=cotangent, weight_in=weight_in, weight_out=weight_out, mask_in=mask_in, mask_out=mask_out)


def spread(weight, mask):
    rows, cols = mask.shape
    blocks = weight.reshape(rows, BLOCK, cols, BLOCK) * mask.astype(weight.dtype)[:, None, :, None]
    return blocks.reshape(weight.shape)


def reference(inputs, cotangent, weight_in, weight_out, mask_in, mask_out):
    sparse_in = spread(weight_in, mask_in)
    sparse_out = spread(weight_out, mask_out)
    pre = jnp.dot(inputs, sparse_in, preferred_element_type=jnp.float32)
    grad_act = lax.dot_general(cotangent, sparse_out, (((1,), (1,)), ((), ())), preferred_element_type=jnp.float32)
    sig = jax.nn.sigmoid(pre)
    act = (pre * sig).astype(jnp.bfloat16)
    grad_pre = (grad_act * sig * (1.0 + pre * (1.0 - sig))).astype(jnp.bfloat16)
    grad_inputs = lax.dot_general(grad_pre, sparse_in, (((1,), (1,)), ((), ())), preferred_element_type=jnp.float32)
    grad_weight_in = lax.dot_general(inputs, grad_pre, (((0,), (0,)), ((), ())), preferred_element_type=jnp.float32)
    grad_weight_out = lax.dot_general(act, cotangent, (((0,), (0,)), ((), ())), preferred_element_type=jnp.float32)
    return grad_inputs, spread(grad_weight_in, mask_in), spread(grad_weight_out, mask_out)
```

```python
import jax
import jax.numpy as jnp
from jax import lax
from jax.sharding import PartitionSpec as P

BLOCK = 128
F16 = jnp.float16
BF16 = jnp.bfloat16
F32 = jnp.float32
PRE_SCALE = 8.0
ACT_SCALE = 64.0


def spread(weight, mask):
    rows, cols = mask.shape
    blocks = weight.reshape(rows, BLOCK, cols, BLOCK) * mask.astype(weight.dtype)[:, None, :, None]
    return blocks.reshape(weight.shape)


def ring(shift, rows):
    return [(r, (r + 2 * shift) % rows) for r in range(rows)]


def reduce_ring(part, scale, rows):
    depth = rows // 2
    chunk = part.shape[0] // depth
    half = chunk // 2
    up_perm, down_perm = ring(1, rows), ring(-1, rows)

    def piece(d, lo=0, hi=chunk):
        d %= depth
        return part[d * chunk + lo : d * chunk + hi] * scale

    far = depth // 2
    up = lax.ppermute(piece(far, 0, half).astype(F16), "row", up_perm)
    down = lax.ppermute(piece(far, half, chunk).astype(F16), "row", down_perm)
    zeros = jnp.zeros((chunk - half, part.shape[1]), F16)
    up = jnp.concatenate([up, zeros], axis=0)
    down = jnp.concatenate([zeros, down], axis=0)
    for d in range(far - 1, 0, -1):
        up = lax.ppermute((piece(d) + up.astype(F32)).astype(F16), "row", up_perm)
        down = lax.ppermute((piece(-d) + down.astype(F32)).astype(F16), "row", down_perm)
    return (piece(0) + up.astype(F32) + down.astype(F32)).astype(F16)


def swap_add(mine, scale, rows):
    other = lax.ppermute(mine, "row", [(r, r ^ 1) for r in range(rows)])
    return (mine.astype(F32) + other.astype(F32)) * (1.0 / scale)


def gather_ring(mine, rows):
    depth = rows // 2
    half = mine.shape[0] // 2
    up_perm, down_perm = ring(1, rows), ring(-1, rows)
    from_below, from_above = [], []
    a = b = mine
    for _ in range(depth // 2 - 1):
        a = lax.ppermute(a, "row", up_perm)
        b = lax.ppermute(b, "row", down_perm)
        from_below.append(a)
        from_above.append(b)
    far = [lax.ppermute(a[:half], "row", up_perm), lax.ppermute(b[half:], "row", down_perm)]
    return jnp.concatenate([mine] + from_above + far + from_below[::-1], axis=0)


def rolled(x, start):
    return lax.dynamic_slice_in_dim(jnp.concatenate([x, x], axis=0), start, x.shape[0], axis=0)


def shards(rows, cols, inputs, cotangent, weight_in, weight_out, mask_in, mask_out):
    tokens = inputs.shape[0] * cols
    z = lax.axis_index("row") // 2
    first = z * (tokens // (rows // 2))
    sparse_in, sparse_out = lax.optimization_barrier(
        (spread(weight_in, mask_in), spread(weight_out, mask_out))
    )
    inputs_all = rolled(lax.all_gather(inputs, "col", axis=0, tiled=True), first)
    cotangent_all = rolled(lax.all_gather(cotangent, "col", axis=0, tiled=True), first)
    pre_part = jnp.dot(inputs_all, sparse_in, preferred_element_type=F32)
    act_part = lax.dot_general(
        cotangent_all, sparse_out, (((1,), (1,)), ((), ())), preferred_element_type=F32
    )
    pre = swap_add(reduce_ring(pre_part, PRE_SCALE, rows), PRE_SCALE, rows)
    grad_act = swap_add(reduce_ring(act_part, ACT_SCALE, rows), ACT_SCALE, rows)
    sig = jax.nn.sigmoid(pre)
    act = (pre * sig).astype(BF16)
    grad_pre = (grad_act * sig * (1.0 + pre * (1.0 - sig))).astype(BF16)
    grad_pre = gather_ring(grad_pre, rows)
    act = gather_ring(act, rows)
    partial = lax.dot_general(
        grad_pre, sparse_in, (((1,), (1,)), ((), ())), preferred_element_type=F32
    ).astype(BF16)
    partial = rolled(partial, tokens - first)
    pieces = lax.all_to_all(partial.reshape(cols, tokens // cols, -1), "col", 0, 0)
    grad_inputs = jnp.sum(pieces.astype(F32), axis=0)
    grad_weight_in = lax.dot_general(
        inputs_all, grad_pre, (((0,), (0,)), ((), ())), preferred_element_type=F32
    )
    grad_weight_out = lax.dot_general(
        act, cotangent_all, (((0,), (0,)), ((), ())), preferred_element_type=F32
    )
    return (grad_inputs, spread(grad_weight_in, mask_in), spread(grad_weight_out, mask_out))


def solution(mesh):
    rows, cols = mesh.shape["row"], mesh.shape["col"]
    return jax.shard_map(
        lambda *args: shards(rows, cols, *args),
        mesh=mesh,
        in_specs=(
            P("col", "row"),
            P("col", "row"),
            P("row", "col"),
            P("col", "row"),
            P("row", "col"),
            P("col", "row"),
        ),
        out_specs=(P("col", "row"), P("row", "col"), P("col", "row")),
        check_vma=False,
    )
```

```python
import jax
import jax.numpy as jnp
from jax import lax
from jax.experimental import pallas as pl
from jax.experimental.pallas import tpu as pltpu
from jax.sharding import PartitionSpec as P

BLOCK = 128
F16 = jnp.float16
BF16 = jnp.bfloat16
F32 = jnp.float32
PRE_SCALE = 8.0
ACT_SCALE = 64.0


def spread(weight, mask):
    rows, cols = mask.shape
    blocks = weight.reshape(rows, BLOCK, cols, BLOCK) * mask.astype(weight.dtype)[:, None, :, None]
    return blocks.reshape(weight.shape)


def ring(shift, rows):
    return [(r, (r + 2 * shift) % rows) for r in range(rows)]


def send(value, shift, rows):
    return lax.ppermute(value, "row", ring(shift, rows))


def swap(value, rows):
    return lax.ppermute(value, "row", [(r, r ^ 1) for r in range(rows)])


def together(*values):
    return lax.optimization_barrier(values)


def chunk_of(stack, index):
    return lax.dynamic_index_in_dim(stack, index % stack.shape[0], 0, keepdims=False)


def gather_kernel(place, *refs):
    depth = len(refs) - 4
    chunks, (weight, stack, pieces, sems) = refs[:depth], refs[depth:]
    z, core = place[0], place[1]
    copies = [
        pltpu.make_async_copy(chunks[d], stack.at[lax.rem(z + d, depth)], sems.at[d])
        for d in range(depth)
    ]
    for copy in copies:
        copy.start()
    for copy in copies:
        copy.wait()
    cols, share, width = pieces.shape
    per_half = depth // 2
    for half in range(2):
        rows = stack[half * per_half : (half + 1) * per_half]
        rows = rows.reshape(per_half * rows.shape[1], rows.shape[2])
        product = lax.dot_general(
            rows, weight[...], (((1,), (1,)), ((), ())), preferred_element_type=F32
        )
        product = product.astype(BF16).reshape(cols // 2, share, width)
        side = core if half == 0 else 1 - core
        for k in range(cols // 2):
            pieces[2 * k + side] = product[k]


def gather_and_multiply(chunks, weight, place, cols):
    depth = len(chunks)
    chunk, hidden = chunks[0].shape
    features = weight.shape[0]
    tokens = depth * chunk
    whole = lambda shape: pl.BlockSpec(shape, lambda i, p: (0,) * len(shape))
    stack, pieces = pl.pallas_call(
        gather_kernel,
        out_shape=(
            jax.ShapeDtypeStruct((depth, chunk, hidden), BF16),
            jax.ShapeDtypeStruct((cols, tokens // cols, features), BF16),
        ),
        grid_spec=pltpu.PrefetchScalarGridSpec(
            num_scalar_prefetch=1,
            grid=(1,),
            in_specs=[pl.BlockSpec(memory_space=pl.ANY)] * depth + [whole(weight.shape)],
            out_specs=(whole((depth, chunk, hidden)), whole((cols, tokens // cols, features))),
            scratch_shapes=[pltpu.SemaphoreType.DMA((depth,))],
        ),
        cost_estimate=pl.CostEstimate(
            flops=2 * tokens * hidden * features, bytes_accessed=8 * tokens * hidden, transcendentals=0
        ),
    )(place, *chunks, weight)
    return stack.reshape(tokens, hidden), pieces


def weight_in_kernel(mask, x, grad, out):
    tile = pl.program_id(0)
    product = lax.dot_general(
        x[...], grad[...], (((0,), (0,)), ((), ())), preferred_element_type=F32
    )
    for i in range(out.shape[0] // BLOCK):
        for j in range(out.shape[1] // BLOCK):
            keep = mask[i, tile * (out.shape[1] // BLOCK) + j].astype(F32)
            at = (slice(i * BLOCK, (i + 1) * BLOCK), slice(j * BLOCK, (j + 1) * BLOCK))
            out[at] = product[at] * keep


def grad_of_weight_in(x, grad, mask, width=512):
    tokens, features = x.shape
    hidden = grad.shape[1]
    return pl.pallas_call(
        weight_in_kernel,
        out_shape=jax.ShapeDtypeStruct((features, hidden), F32),
        grid=(hidden // width,),
        in_specs=[
            pl.BlockSpec(memory_space=pltpu.SMEM),
            pl.BlockSpec((tokens, features), lambda i: (0, 0)),
            pl.BlockSpec((tokens, width), lambda i: (0, i)),
        ],
        out_specs=pl.BlockSpec((features, width), lambda i: (0, i)),
        cost_estimate=pl.CostEstimate(
            flops=2 * tokens * hidden * features, bytes_accessed=8 * features * hidden, transcendentals=0
        ),
    )(mask, x, grad)


def weight_out_kernel(place, *refs):
    depth = len(refs) - 5
    chunks, (mask, cot, out, stack, sems) = refs[:depth], refs[depth:]
    tile = pl.program_id(0)
    z = place[0]

    @pl.when(tile == 0)
    def _():
        copies = [
            pltpu.make_async_copy(chunks[d], stack.at[lax.rem(z + d, depth)], sems.at[d])
            for d in range(depth)
        ]
        for copy in copies:
            copy.start()
        for copy in copies:
            copy.wait()

    height = out.shape[0]
    act = stack[:, :, pl.ds(pl.multiple_of(tile * height, BLOCK), height)]
    act = act.reshape(depth * act.shape[1], height)
    product = lax.dot_general(
        act, cot[...], (((0,), (0,)), ((), ())), preferred_element_type=F32
    )
    for i in range(height // BLOCK):
        for j in range(out.shape[1] // BLOCK):
            keep = mask[tile * (height // BLOCK) + i, j].astype(F32)
            at = (slice(i * BLOCK, (i + 1) * BLOCK), slice(j * BLOCK, (j + 1) * BLOCK))
            out[at] = product[at] * keep


def grad_of_weight_out(chunks, cot, mask, place, height=512):
    depth = len(chunks)
    chunk, hidden = chunks[0].shape
    tokens, features = cot.shape
    return pl.pallas_call(
        weight_out_kernel,
        out_shape=jax.ShapeDtypeStruct((hidden, features), F32),
        grid_spec=pltpu.PrefetchScalarGridSpec(
            num_scalar_prefetch=1,
            grid=(hidden // height,),
            in_specs=[pl.BlockSpec(memory_space=pl.ANY)] * depth
            + [
                pl.BlockSpec(memory_space=pltpu.SMEM),
                pl.BlockSpec((tokens, features), lambda i, p: (0, 0)),
            ],
            out_specs=pl.BlockSpec((height, features), lambda i, p: (i, 0)),
            scratch_shapes=[
                pltpu.VMEM((depth, chunk, hidden), BF16),
                pltpu.SemaphoreType.DMA((depth,)),
            ],
        ),
        cost_estimate=pl.CostEstimate(
            flops=2 * tokens * hidden * features, bytes_accessed=8 * features * hidden, transcendentals=0
        ),
    )(place, *chunks, mask, cot)


def shards(rows, cols, inputs, cotangent, weight_in, weight_out, mask_in, mask_out):
    share, width = inputs.shape
    chips = cols // 2
    tokens = share * cols
    depth = rows // 2
    far = depth // 2
    same_core = [[2 * k + i for k in range(chips)] for i in range(2)]
    other_core = [(c, c ^ 1) for c in range(cols)]
    z = lax.axis_index("row") // 2
    place = jnp.stack([z, lax.axis_index("col") % 2]).astype(jnp.int32)

    both = jnp.concatenate([inputs, cotangent], axis=1)
    both = jnp.broadcast_to(both[None], (chips, share, 2 * width))
    mine = lax.all_to_all(both, "col", 0, 0, axis_index_groups=same_core)
    both = jnp.concatenate([mine, lax.ppermute(mine, "col", other_core)], axis=0)
    both = both.reshape(tokens, 2 * width)
    inputs_all, cotangent_all = both[:, :width], both[:, width:]
    sparse_in, sparse_out = together(spread(weight_in, mask_in), spread(weight_out, mask_out))
    pre_part = jnp.dot(inputs_all, sparse_in, preferred_element_type=F32)
    act_part = lax.dot_general(
        cotangent_all, sparse_out, (((1,), (1,)), ((), ())), preferred_element_type=F32
    )
    pre_part = pre_part.reshape(depth, tokens // depth, -1)
    act_part = act_part.reshape(depth, tokens // depth, -1)
    inputs_all, cotangent_all = together(inputs_all, cotangent_all)

    def p(d):
        return chunk_of(pre_part, z + d) * PRE_SCALE

    def g(d):
        return chunk_of(act_part, z + d + depth) * ACT_SCALE

    pu, pd = p(far).astype(F16), p(depth - far + 1).astype(F16)
    gu, gd = g(far - 1).astype(F16), g(-far).astype(F16)
    for step in range(1, far):
        pu, pd = together(send(pu, 1, rows), send(pd, -1, rows))
        pu = (p(far - step) + pu.astype(F32)).astype(F16)
        if step < far - 1:
            pd = (p(depth - far + 1 + step) + pd.astype(F32)).astype(F16)
        gu, gd = together(send(gu, 1, rows), send(gd, -1, rows))
        if step < far - 1:
            gu = (g(far - 1 - step) + gu.astype(F32)).astype(F16)
        gd = (g(-far + step) + gd.astype(F32)).astype(F16)
    pu = send(pu, 1, rows)
    gd = send(gd, -1, rows)
    pre = (p(0) + pu.astype(F32) + pd.astype(F32)).astype(F16)
    pre = (pre.astype(F32) + swap(pre, rows).astype(F32)) * (1.0 / PRE_SCALE)
    grad_act = (g(0) + gu.astype(F32) + gd.astype(F32)).astype(F16)
    grad_act = (grad_act.astype(F32) + swap(grad_act, rows).astype(F32)) * (1.0 / ACT_SCALE)
    sig = jax.nn.sigmoid(pre)
    act = (pre * sig).astype(BF16)
    grad_pre = (grad_act * sig * (1.0 + pre * (1.0 - sig))).astype(BF16)

    acts, grads = {0: act}, {0: grad_pre}
    au = ad = act
    gu = gd = grad_pre
    for step in range(1, far + 1):
        au = acts[depth - step] = send(au, 1, rows)
        if step < far:
            ad = acts[step] = send(ad, -1, rows)
            gu = grads[depth - step] = send(gu, 1, rows)
        gd = grads[step] = send(gd, -1, rows)
    acts = [acts[d] for d in range(depth)]
    grads = [grads[d] for d in range(depth)]

    grad_pre, pieces = gather_and_multiply(grads, sparse_in, place, cols)
    pieces = lax.all_to_all(pieces, "col", 0, 0)
    grad_inputs = jnp.sum(pieces.astype(F32), axis=0)
    grad_weight_in = grad_of_weight_in(inputs_all, grad_pre, mask_in)
    grad_weight_out = grad_of_weight_out(acts, cotangent_all, mask_out, place)
    return (grad_inputs, grad_weight_in, grad_weight_out)


def solution(mesh):
    rows, cols = mesh.shape["row"], mesh.shape["col"]
    return jax.shard_map(
        lambda *args: shards(rows, cols, *args),
        mesh=mesh,
        in_specs=(
            P("col", "row"),
            P("col", "row"),
            P("row", "col"),
            P("col", "row"),
            P("row", "col"),
            P("col", "row"),
        ),
        out_specs=(P("col", "row"), P("row", "col"), P("col", "row")),
        check_vma=False,
    )
```

```python
import jax
import jax.numpy as jnp
from jax import lax
from jax.experimental import pallas as pl
from jax.experimental.pallas import tpu as pltpu
from jax.sharding import PartitionSpec as P

BLOCK = 128
F16 = jnp.float16
BF16 = jnp.bfloat16
F32 = jnp.float32
PRE_SCALE = 8.0
ACT_SCALE = 64.0


def spread(weight, mask):
    rows, cols = mask.shape
    blocks = weight.reshape(rows, BLOCK, cols, BLOCK) * mask.astype(weight.dtype)[:, None, :, None]
    return blocks.reshape(weight.shape)


def ring(shift, rows):
    return [(r, (r + 2 * shift) % rows) for r in range(rows)]


def send(value, shift, rows):
    return lax.ppermute(value, "row", ring(shift, rows))


def swap(value, rows):
    return lax.ppermute(value, "row", [(r, r ^ 1) for r in range(rows)])


def together(*values):
    return lax.optimization_barrier(values)


def chunk_of(stack, index):
    return lax.dynamic_index_in_dim(stack, index % stack.shape[0], 0, keepdims=False)


def weight_in_kernel(mask, x, grad, out):
    tile = pl.program_id(0)
    product = lax.dot_general(
        x[...], grad[...], (((0,), (0,)), ((), ())), preferred_element_type=F32
    )
    for i in range(out.shape[0] // BLOCK):
        for j in range(out.shape[1] // BLOCK):
            keep = mask[i, tile * (out.shape[1] // BLOCK) + j].astype(F32)
            at = (slice(i * BLOCK, (i + 1) * BLOCK), slice(j * BLOCK, (j + 1) * BLOCK))
            out[at] = product[at] * keep


def grad_of_weight_in(x, grad, mask, width=1024):
    tokens, features = x.shape
    hidden = grad.shape[1]
    return pl.pallas_call(
        weight_in_kernel,
        out_shape=jax.ShapeDtypeStruct((features, hidden), F32),
        grid=(hidden // width,),
        in_specs=[
            pl.BlockSpec(memory_space=pltpu.SMEM),
            pl.BlockSpec((tokens, features), lambda i: (0, 0)),
            pl.BlockSpec((tokens, width), lambda i: (0, i)),
        ],
        out_specs=pl.BlockSpec((features, width), lambda i: (0, i)),
        cost_estimate=pl.CostEstimate(
            flops=2 * tokens * hidden * features, bytes_accessed=8 * features * hidden, transcendentals=0
        ),
    )(mask, x, grad)


def shards(rows, cols, inputs, cotangent, weight_in, weight_out, mask_in, mask_out):
    share, width = inputs.shape
    chips = cols // 2
    tokens = share * cols
    depth = rows // 2
    far = depth // 2
    same_core = [[2 * k + i for k in range(chips)] for i in range(2)]
    other_core = [(c, c ^ 1) for c in range(cols)]
    z = lax.axis_index("row") // 2
    first_core = lax.axis_index("col") % 2 == 0

    mine = jnp.concatenate([inputs, cotangent], axis=1)
    mine = jnp.broadcast_to(mine[None], (chips, share, 2 * width))
    mine = lax.all_to_all(mine, "col", 0, 0, axis_index_groups=same_core)
    other = lax.ppermute(mine, "col", other_core)
    both = jnp.stack(
        [jnp.where(first_core, mine, other), jnp.where(first_core, other, mine)], axis=1
    )
    both = both.reshape(tokens, 2 * width)
    inputs_all, cotangent_all = both[:, :width], both[:, width:]
    sparse_in, sparse_out = together(spread(weight_in, mask_in), spread(weight_out, mask_out))
    pre_part = jnp.dot(inputs_all, sparse_in, preferred_element_type=F32)
    act_part = lax.dot_general(
        cotangent_all, sparse_out, (((1,), (1,)), ((), ())), preferred_element_type=F32
    )
    pre_part = pre_part.reshape(depth, tokens // depth, -1)
    act_part = act_part.reshape(depth, tokens // depth, -1)
    inputs_all, cotangent_all = together(inputs_all, cotangent_all)

    def p(d):
        return chunk_of(pre_part, z + d) * PRE_SCALE

    def g(d):
        return chunk_of(act_part, z + d + depth) * ACT_SCALE

    pu, pd = p(far).astype(F16), p(depth - far + 1).astype(F16)
    gu, gd = g(far - 1).astype(F16), g(-far).astype(F16)
    for step in range(1, far):
        pu, pd = together(send(pu, 1, rows), send(pd, -1, rows))
        pu = (p(far - step) + pu.astype(F32)).astype(F16)
        if step < far - 1:
            pd = (p(depth - far + 1 + step) + pd.astype(F32)).astype(F16)
        gu, gd, _ = together(send(gu, 1, rows), send(gd, -1, rows), pu)
        if step < far - 1:
            gu = (g(far - 1 - step) + gu.astype(F32)).astype(F16)
        gd = (g(-far + step) + gd.astype(F32)).astype(F16)
    pu = send(pu, 1, rows)
    gd = send(gd, -1, rows)
    pre = (p(0) + pu.astype(F32) + pd.astype(F32)).astype(F16)
    pre = (pre.astype(F32) + swap(pre, rows).astype(F32)) * (1.0 / PRE_SCALE)
    grad_act = (g(0) + gu.astype(F32) + gd.astype(F32)).astype(F16)
    grad_act = (grad_act.astype(F32) + swap(grad_act, rows).astype(F32)) * (1.0 / ACT_SCALE)
    sig = jax.nn.sigmoid(pre)
    act, slope = together((pre * sig).astype(BF16), sig * (1.0 + pre * (1.0 - sig)))
    au, ad = send(act, 1, rows), send(act, -1, rows)
    au, ad = together(au, ad)
    grad_pre = (grad_act * slope).astype(BF16)

    acts, grads = {0: act, depth - 1: au, 1: ad}, {0: grad_pre}
    gu = gd = grad_pre
    for step in range(1, far):
        gu, gd = together(send(gu, 1, rows), send(gd, -1, rows))
        grads[depth - step], grads[step] = gu, gd
        au = acts[depth - step - 1] = send(au, 1, rows)
        if step < far - 1:
            ad = acts[step + 1] = send(ad, -1, rows)
            au, ad = together(au, ad)
    grads[far] = send(gd, -1, rows)

    chunk = tokens // depth
    gathered = jnp.zeros((depth, chunk, grad_pre.shape[1]), BF16)
    for d in [0] + [d for k in range(1, far) for d in (k, depth - k)] + [far]:
        gathered = lax.dynamic_update_index_in_dim(gathered, grads[d], (z + d) % depth, 0)
    (gathered,) = together(gathered.reshape(tokens, -1))
    partial = lax.dot_general(
        gathered, sparse_in, (((1,), (1,)), ((), ())), preferred_element_type=F32
    )
    pieces = partial.astype(BF16).reshape(cols, share, width)
    pieces = lax.all_to_all(pieces, "col", 0, 0)
    grad_inputs = jnp.sum(pieces.astype(F32), axis=0)
    grad_weight_in = grad_of_weight_in(inputs_all, gathered, mask_in)
    turned = cotangent_all.reshape(depth, chunk, width)
    turned = lax.dynamic_slice_in_dim(jnp.concatenate([turned, turned]), z, depth, axis=0)
    act, turned = together(
        jnp.concatenate([acts[d] for d in range(depth)], axis=0), turned.reshape(tokens, width)
    )
    grad_weight_out = lax.dot_general(
        act, turned, (((0,), (0,)), ((), ())), preferred_element_type=F32
    )
    return (grad_inputs, grad_weight_in, spread(grad_weight_out, mask_out))


def solution(mesh):
    rows, cols = mesh.shape["row"], mesh.shape["col"]
    return jax.shard_map(
        lambda *args: shards(rows, cols, *args),
        mesh=mesh,
        in_specs=(
            P("col", "row"),
            P("col", "row"),
            P("row", "col"),
            P("col", "row"),
            P("row", "col"),
            P("col", "row"),
        ),
        out_specs=(P("col", "row"), P("row", "col"), P("col", "row")),
        check_vma=False,
    )
```

```python
import jax
import jax.numpy as jnp
from jax import lax
from jax.experimental import pallas as pl
from jax.experimental.pallas import tpu as pltpu
from jax.sharding import PartitionSpec as P

BLOCK = 128
F16 = jnp.float16
BF16 = jnp.bfloat16
F32 = jnp.float32
PRE_SCALE = 8.0
ACT_SCALE = 64.0


def spread(weight, mask):
    rows, cols = mask.shape
    blocks = weight.reshape(rows, BLOCK, cols, BLOCK) * mask.astype(weight.dtype)[:, None, :, None]
    return blocks.reshape(weight.shape)


def ring(shift, rows):
    return [(r, (r + 2 * shift) % rows) for r in range(rows)]


def send(value, shift, rows):
    return lax.ppermute(value, "row", ring(shift, rows))


def swap(value, rows):
    return lax.ppermute(value, "row", [(r, r ^ 1) for r in range(rows)])


def together(*values):
    return lax.optimization_barrier(values)


def chunk_of(stack, index):
    return lax.dynamic_index_in_dim(stack, index % stack.shape[0], 0, keepdims=False)


def weight_in_kernel(mask, x, grad, out):
    tile = pl.program_id(0)
    product = lax.dot_general(
        x[...], grad[...], (((0,), (0,)), ((), ())), preferred_element_type=F32
    )
    for i in range(out.shape[0] // BLOCK):
        for j in range(out.shape[1] // BLOCK):
            keep = mask[i, tile * (out.shape[1] // BLOCK) + j].astype(F32)
            at = (slice(i * BLOCK, (i + 1) * BLOCK), slice(j * BLOCK, (j + 1) * BLOCK))
            out[at] = product[at] * keep


def grad_of_weight_in(x, grad, mask, width=1024):
    tokens, features = x.shape
    hidden = grad.shape[1]
    return pl.pallas_call(
        weight_in_kernel,
        out_shape=jax.ShapeDtypeStruct((features, hidden), F32),
        grid=(hidden // width,),
        in_specs=[
            pl.BlockSpec(memory_space=pltpu.SMEM),
            pl.BlockSpec((tokens, features), lambda i: (0, 0)),
            pl.BlockSpec((tokens, width), lambda i: (0, i)),
        ],
        out_specs=pl.BlockSpec((features, width), lambda i: (0, i)),
        cost_estimate=pl.CostEstimate(
            flops=2 * tokens * hidden * features, bytes_accessed=8 * features * hidden, transcendentals=0
        ),
    )(mask, x, grad)


def shards(rows, cols, inputs, cotangent, weight_in, weight_out, mask_in, mask_out):
    share, width = inputs.shape
    chips = cols // 2
    tokens = share * cols
    depth = rows // 2
    far = depth // 2
    same_core = [[2 * k + i for k in range(chips)] for i in range(2)]
    other_core = [(c, c ^ 1) for c in range(cols)]
    z = lax.axis_index("row") // 2
    first_core = lax.axis_index("col") % 2 == 0

    mine = jnp.concatenate([inputs, cotangent], axis=1)
    mine = jnp.broadcast_to(mine[None], (chips, share, 2 * width))
    mine = lax.all_to_all(mine, "col", 0, 0, axis_index_groups=same_core)
    other = lax.ppermute(mine, "col", other_core)
    both = jnp.stack(
        [jnp.where(first_core, mine, other), jnp.where(first_core, other, mine)], axis=1
    )
    both = both.reshape(tokens, 2 * width)
    inputs_all, cotangent_all = both[:, :width], both[:, width:]
    (sparse_in,) = together(spread(weight_in, mask_in))
    (sparse_out,) = together(spread(weight_out, mask_out))
    pre_part = jnp.dot(inputs_all, sparse_in, preferred_element_type=F32)
    act_part = lax.dot_general(
        cotangent_all, sparse_out, (((1,), (1,)), ((), ())), preferred_element_type=F32
    )
    pre_part = pre_part.reshape(depth, tokens // depth, -1)
    act_part = act_part.reshape(depth, tokens // depth, -1)
    inputs_all, cotangent_all = together(inputs_all, cotangent_all)

    def p(d):
        return chunk_of(pre_part, z + d) * PRE_SCALE

    def g(d):
        return chunk_of(act_part, z + d + depth) * ACT_SCALE

    pu, pd = p(far).astype(F16), p(depth - far + 1).astype(F16)
    gu, gd = g(far - 1).astype(F16), g(-far).astype(F16)
    for step in range(1, far):
        pu, pd = together(send(pu, 1, rows), send(pd, -1, rows))
        pu = (p(far - step) + pu.astype(F32)).astype(F16)
        if step < far - 1:
            pd = (p(depth - far + 1 + step) + pd.astype(F32)).astype(F16)
        gu, gd, _ = together(send(gu, 1, rows), send(gd, -1, rows), pu)
        if step < far - 1:
            gu = (g(far - 1 - step) + gu.astype(F32)).astype(F16)
        gd = (g(-far + step) + gd.astype(F32)).astype(F16)
    pu = send(pu, 1, rows)
    gd = send(gd, -1, rows)
    pre = (p(0) + pu.astype(F32) + pd.astype(F32)).astype(F16)
    pre = (pre.astype(F32) + swap(pre, rows).astype(F32)) * (1.0 / PRE_SCALE)
    grad_act = (g(0) + gu.astype(F32) + gd.astype(F32)).astype(F16)
    grad_act = (grad_act.astype(F32) + swap(grad_act, rows).astype(F32)) * (1.0 / ACT_SCALE)
    sig = jax.nn.sigmoid(pre)
    act, slope = together((pre * sig).astype(BF16), sig * (1.0 + pre * (1.0 - sig)))
    au, ad = send(act, 1, rows), send(act, -1, rows)
    au, ad = together(au, ad)
    grad_pre = (grad_act * slope).astype(BF16)

    acts, grads = {0: act, depth - 1: au, 1: ad}, {0: grad_pre}
    gu = gd = grad_pre
    for step in range(1, far):
        gu, gd = together(send(gu, 1, rows), send(gd, -1, rows))
        grads[depth - step], grads[step] = gu, gd
        au = acts[depth - step - 1] = send(au, 1, rows)
        if step < far - 1:
            ad = acts[step + 1] = send(ad, -1, rows)
            au, ad = together(au, ad)
    grads[far] = send(gd, -1, rows)

    chunk = tokens // depth
    gathered = jnp.zeros((depth, chunk, grad_pre.shape[1]), BF16)
    for d in [0] + [d for k in range(1, far) for d in (k, depth - k)] + [far]:
        gathered = lax.dynamic_update_index_in_dim(gathered, grads[d], (z + d) % depth, 0)
    (gathered,) = together(gathered.reshape(tokens, -1))
    partial = lax.dot_general(
        gathered, sparse_in, (((1,), (1,)), ((), ())), preferred_element_type=F32
    )
    pieces = partial.astype(BF16).reshape(cols, share, width)
    pieces = lax.all_to_all(pieces, "col", 0, 0)
    grad_inputs = jnp.sum(pieces.astype(F32), axis=0)
    grad_weight_in = grad_of_weight_in(inputs_all, gathered, mask_in)
    turned = cotangent_all.reshape(depth, chunk, width)
    turned = lax.dynamic_slice_in_dim(jnp.concatenate([turned, turned]), z, depth, axis=0)
    act = jnp.zeros((depth, chunk, act.shape[1]), BF16)
    for d in [0] + [d for k in range(1, far) for d in (k, depth - k)] + [far]:
        act = lax.dynamic_update_index_in_dim(act, acts[d], d, 0)
    act, turned = together(act.reshape(tokens, -1), turned.reshape(tokens, width))
    grad_weight_out = lax.dot_general(
        act, turned, (((0,), (0,)), ((), ())), preferred_element_type=F32
    )
    return (grad_inputs, grad_weight_in, spread(grad_weight_out, mask_out))


def solution(mesh):
    rows, cols = mesh.shape["row"], mesh.shape["col"]
    return jax.shard_map(
        lambda *args: shards(rows, cols, *args),
        mesh=mesh,
        in_specs=(
            P("col", "row"),
            P("col", "row"),
            P("row", "col"),
            P("col", "row"),
            P("row", "col"),
            P("col", "row"),
        ),
        out_specs=(P("col", "row"), P("row", "col"), P("col", "row")),
        check_vma=False,
    )
```

```python
import jax
import jax.numpy as jnp
from jax import lax
from jax.experimental import pallas as pl
from jax.experimental.pallas import tpu as pltpu
from jax.sharding import PartitionSpec as P

BLOCK = 128
F16 = jnp.float16
BF16 = jnp.bfloat16
F32 = jnp.float32
PRE_SCALE = 8.0
ACT_SCALE = 64.0


def spread(weight, mask):
    rows, cols = mask.shape
    blocks = weight.reshape(rows, BLOCK, cols, BLOCK) * mask.astype(weight.dtype)[:, None, :, None]
    return blocks.reshape(weight.shape)


def ring(shift, rows):
    return [(r, (r + 2 * shift) % rows) for r in range(rows)]


def send(value, shift, rows):
    return lax.ppermute(value, "row", ring(shift, rows))


def swap(value, rows):
    return lax.ppermute(value, "row", [(r, r ^ 1) for r in range(rows)])


def together(*values):
    return lax.optimization_barrier(values)


def chunk_of(stack, index):
    return lax.dynamic_index_in_dim(stack, index % stack.shape[0], 0, keepdims=False)


def weight_in_kernel(mask, x, grad, out):
    tile = pl.program_id(0)
    product = lax.dot_general(
        x[...], grad[...], (((0,), (0,)), ((), ())), preferred_element_type=F32
    )
    for i in range(out.shape[0] // BLOCK):
        for j in range(out.shape[1] // BLOCK):
            keep = mask[i, tile * (out.shape[1] // BLOCK) + j].astype(F32)
            at = (slice(i * BLOCK, (i + 1) * BLOCK), slice(j * BLOCK, (j + 1) * BLOCK))
            out[at] = product[at] * keep


def grad_of_weight_in(x, grad, mask, width=1024):
    tokens, features = x.shape
    hidden = grad.shape[1]
    return pl.pallas_call(
        weight_in_kernel,
        out_shape=jax.ShapeDtypeStruct((features, hidden), F32),
        grid=(hidden // width,),
        in_specs=[
            pl.BlockSpec(memory_space=pltpu.SMEM),
            pl.BlockSpec((tokens, features), lambda i: (0, 0)),
            pl.BlockSpec((tokens, width), lambda i: (0, i)),
        ],
        out_specs=pl.BlockSpec((features, width), lambda i: (0, i)),
        cost_estimate=pl.CostEstimate(
            flops=2 * tokens * hidden * features, bytes_accessed=8 * features * hidden, transcendentals=0
        ),
    )(mask, x, grad)


def shards(rows, cols, inputs, cotangent, weight_in, weight_out, mask_in, mask_out):
    share, width = inputs.shape
    chips = cols // 2
    tokens = share * cols
    depth = rows // 2
    far = depth // 2
    same_core = [[2 * k + i for k in range(chips)] for i in range(2)]
    other_core = [(c, c ^ 1) for c in range(cols)]
    z = lax.axis_index("row") // 2
    first_core = lax.axis_index("col") % 2 == 0

    mine = jnp.concatenate([inputs, cotangent], axis=1)
    mine = jnp.broadcast_to(mine[None], (chips, share, 2 * width))
    mine = lax.all_to_all(mine, "col", 0, 0, axis_index_groups=same_core)
    other = lax.ppermute(mine, "col", other_core)
    both = jnp.stack(
        [jnp.where(first_core, mine, other), jnp.where(first_core, other, mine)], axis=1
    )
    both = both.reshape(tokens, 2 * width)
    inputs_all, cotangent_all = both[:, :width], both[:, width:]
    (sparse_in,) = together(spread(weight_in, mask_in))
    (sparse_out,) = together(spread(weight_out, mask_out))
    pre_part = jnp.dot(inputs_all, sparse_in, preferred_element_type=F32)
    act_part = lax.dot_general(
        cotangent_all, sparse_out, (((1,), (1,)), ((), ())), preferred_element_type=F32
    )
    pre_part = pre_part.reshape(depth, tokens // depth, -1)
    act_part = act_part.reshape(depth, tokens // depth, -1)

    def p(d):
        return chunk_of(pre_part, z + d) * PRE_SCALE

    def g(d):
        return chunk_of(act_part, z + d + depth) * ACT_SCALE

    pu, pd = p(far).astype(F16), p(depth - far + 1).astype(F16)
    gu, gd = g(far - 1).astype(F16), g(-far).astype(F16)
    for step in range(1, far):
        pu, pd = together(send(pu, 1, rows), send(pd, -1, rows))
        pu = (p(far - step) + pu.astype(F32)).astype(F16)
        if step < far - 1:
            pd = (p(depth - far + 1 + step) + pd.astype(F32)).astype(F16)
        gu, gd, _ = together(send(gu, 1, rows), send(gd, -1, rows), pu)
        if step < far - 1:
            gu = (g(far - 1 - step) + gu.astype(F32)).astype(F16)
        gd = (g(-far + step) + gd.astype(F32)).astype(F16)
    inputs_all, cotangent_all, _ = together(inputs_all, cotangent_all, pu)
    pu = send(pu, 1, rows)
    gd = send(gd, -1, rows)
    pre = (p(0) + pu.astype(F32) + pd.astype(F32)).astype(F16)
    pre = (pre.astype(F32) + swap(pre, rows).astype(F32)) * (1.0 / PRE_SCALE)
    grad_act = (g(0) + gu.astype(F32) + gd.astype(F32)).astype(F16)
    grad_act = (grad_act.astype(F32) + swap(grad_act, rows).astype(F32)) * (1.0 / ACT_SCALE)
    sig = jax.nn.sigmoid(pre)
    act, slope = together((pre * sig).astype(BF16), sig * (1.0 + pre * (1.0 - sig)))
    au, ad = send(act, 1, rows), send(act, -1, rows)
    au, ad = together(au, ad)
    grad_pre = (grad_act * slope).astype(BF16)

    acts, grads = {0: act, depth - 1: au, 1: ad}, {0: grad_pre}
    gu = gd = grad_pre
    for step in range(1, far):
        gu, gd = together(send(gu, 1, rows), send(gd, -1, rows))
        grads[depth - step], grads[step] = gu, gd
        au = acts[depth - step - 1] = send(au, 1, rows)
        if step < far - 1:
            ad = acts[step + 1] = send(ad, -1, rows)
            au, ad = together(au, ad)
    grads[far] = send(gd, -1, rows)

    chunk = tokens // depth
    gathered = jnp.zeros((depth, chunk, grad_pre.shape[1]), BF16)
    for d in [0] + [d for k in range(1, far) for d in (k, depth - k)] + [far]:
        gathered = lax.dynamic_update_index_in_dim(gathered, grads[d], (z + d) % depth, 0)
    (gathered,) = together(gathered.reshape(tokens, -1))
    partial = lax.dot_general(
        gathered, sparse_in, (((1,), (1,)), ((), ())), preferred_element_type=F32
    )
    pieces = partial.astype(BF16).reshape(cols, share, width)
    pieces = lax.all_to_all(pieces, "col", 0, 0)
    grad_inputs = jnp.sum(pieces.astype(F32), axis=0)
    grad_weight_in = grad_of_weight_in(inputs_all, gathered, mask_in)
    turned = cotangent_all.reshape(depth, chunk, width)
    turned = lax.dynamic_slice_in_dim(jnp.concatenate([turned, turned]), z, depth, axis=0)
    act = jnp.zeros((depth, chunk, act.shape[1]), BF16)
    for d in [0] + [d for k in range(1, far) for d in (k, depth - k)] + [far]:
        act = lax.dynamic_update_index_in_dim(act, acts[d], d, 0)
    act, turned = together(act.reshape(tokens, -1), turned.reshape(tokens, width))
    grad_weight_out = lax.dot_general(
        act, turned, (((0,), (0,)), ((), ())), preferred_element_type=F32
    )
    return (grad_inputs, grad_weight_in, spread(grad_weight_out, mask_out))


def solution(mesh):
    rows, cols = mesh.shape["row"], mesh.shape["col"]
    return jax.shard_map(
        lambda *args: shards(rows, cols, *args),
        mesh=mesh,
        in_specs=(
            P("col", "row"),
            P("col", "row"),
            P("row", "col"),
            P("col", "row"),
            P("row", "col"),
            P("col", "row"),
        ),
        out_specs=(P("col", "row"), P("row", "col"), P("col", "row")),
        check_vma=False,
    )
```
